512 devices in a mesh: gx: 8 (over y), gy: 16 (over z, core), gz: 4 (over x).
Axes of the slice: x: 4, y: 8, z: 8, core: 2. Of those that a mesh axis runs over, the one named last changes fastest.
Arguments:
- eri: bfloat16 [16384, 256, 256], P(('gx', 'gy', 'gz')), may hold values from -0.375 to 0.375
- owner: int32 [16384, 1], P(('gx', 'gy', 'gz')), may hold values from 0 to 7; in each aligned block of 32 rows (0 to 31, 32 to 63, ...) at most 8 rows name the same one
- quartet: int32 [16384, 4], P(('gx', 'gy', 'gz')), may hold values from 0 to 191, as said below
- significance: int32 [16384], P(('gx', 'gy', 'gz')), may hold values 0 or 1
- density: bfloat16 [3072, 3072], P('gy'), may hold values from -6 to 6
Outputs:
- exchange: float32 [3072, 3072], P('gx', 'gy')
The draws below stay inside these ranges and needn't reach their ends.
Inputs may be any that keep to these rules, and one draw needn't show every extreme that they name: Among the 32 tiles of one device (aligned blocks of 32 rows), no owner value is named more than 8 times, and in some blocks one is named exactly 8 times. `quartet`: column 0 lies in 0 to 5, column 1 in 0 to 191, column 2 in 0 to 11, column 3 in 0 to 191.
All inputs are finite; a program needn't handle non-finite values. No bound on the sum of `significance` on one device may be relied on, other than what follows from the above.
Results may differ from the reference program's by a relative error of at most 0.0003.
Values sent between devices are 32-bit elements; how exact they have to be, the bound alone decides.
A program may use at most 64 MiB of HBM per device.

```python
import math
import jax
import jax.numpy as jnp
import numpy as np
from jax import lax

NBAS = 3072
SHELL = 16
TILES_DEV = 32
NSH = 192
ROWSH = 6
DSLAB = 12
CAP = 8
TILES = 16384
N_GX = 8
N_GY = 16
N_GZ = 4


def draw_quartet(key, part):
    upper = jnp.array([ROWSH, NSH, DSLAB, NSH], dtype=jnp.int32)
    return jax.random.randint(key, (TILES, 4), 0, upper, dtype=jnp.int32)


def touch_ends(values, key, least, largest):
    dims = values.shape
    spot = [jax.random.randint(jax.random.fold_in(key, axis), (), 0, dims[axis]) for axis in range(len(dims))]
    values = values.at[tuple(spot)].set(least)
    longest = dims.index(max(dims))
    spot[longest] = (spot[longest] + 1) % dims[longest]
    return values.at[tuple(spot)].set(largest)


def level_of(key, extent, split, low, high):
    factor_of, own = 1.0, jax.random.fold_in(key, 6)
    for dim, parts in split:
        heights = jnp.exp(jax.random.uniform(jax.random.fold_in(own, dim), (parts,), jnp.float32, low / len(split), high / len(split)))
        factor_of = factor_of * jnp.repeat(heights, extent[dim] // parts).reshape([-1 if axis == dim else 1 for axis in range(len(extent))])
    return factor_of


def assign_block(rng, own, number, rows, count, top, limit, slope):
    order = jax.random.permutation(rng, count)
    crowded, ordinary = portions_of(count, rows * top, limit, slope, True), portions_of(count, rows * top, limit, slope, False)
    places = jnp.arange(count)

    def named(lengths, turn):
        used = int((lengths > 0).sum())
        fixed = max(1, used // 4)
        moved = fixed + (places - fixed + turn * (used - fixed)) % max(1, count - fixed)
        return jnp.zeros((count,), jnp.int32).at[order[jnp.where(places < fixed, places, moved)]].set(jnp.asarray(lengths, jnp.int32))

    lengths = jnp.where(number % 4 == 0, named(crowded, number // 4), named(ordinary, number - number // 4 - 1))
    mixed = jax.random.permutation(jax.random.fold_in(own, 3), count)
    donor, sink = mixed[0:count // 2 * 2:2], mixed[1:count // 2 * 2:2]
    room = jnp.minimum(lengths[donor] - 1, limit - lengths[sink]) // 2
    room = jnp.where((donor == order[0]) | (sink == order[0]) | (lengths[sink] == 0), 0, jnp.maximum(room, 0))
    moved = jax.random.randint(jax.random.fold_in(own, 4), (count // 2,), 0, 1 << 20) % (room + 1)
    lengths = lengths.at[donor].add(-moved).at[sink].add(moved)
    labels = jnp.searchsorted(jnp.cumsum(lengths), jnp.arange(rows * top), side="right").astype(jnp.int32)
    table = labels.reshape(top, rows).T
    table = table[jax.random.permutation(jax.random.fold_in(own, 1), rows)]
    turn = jax.random.randint(jax.random.fold_in(own, 2), (rows, 1), 0, top)
    return jnp.take_along_axis(table, (jnp.arange(top)[None, :] + turn) % top, axis=1)


def portions_of(amount, total, bound, slope, full):
    portions = [(1 << 20) // math.isqrt(standing ** slope) + 1 for standing in range(1, amount + 1)]
    largest = bound if full else min(bound, max(-(-total // amount), total * portions[0] // sum(portions)))
    least = 1 if total - largest >= amount - 1 else 0
    holding, surplus = [largest] + [least] * (amount - 1), total - largest - least * (amount - 1)
    while surplus > 0:
        free = [i for i in range(1, amount) if holding[i] < largest] or [i for i in range(1, amount) if holding[i] < bound]
        mass, budget = sum([portions[i] for i in free]), surplus
        for i in free:
            extra = min(bound - holding[i], max(1, budget * portions[i] // mass), surplus)
            holding[i] = holding[i] + extra
            surplus = surplus - extra
    return np.array(holding)


def noise(key, extent, scale, bound, cuts=(), kind=jnp.bfloat16):
    drawn = jax.random.normal(key, extent, jnp.float32) * scale
    if len(cuts) > 0:
        drawn = level_of(key, extent, cuts, -0.22, 0.18) * drawn
    return jnp.clip(drawn, min=-bound, max=bound).astype(kind)


def setup_inputs(seed: int = 0) -> dict:
    seeds = jax.random.split(jax.random.key(seed), 6)
    eri = noise(seeds[0], (TILES, SHELL * SHELL, SHELL * SHELL), (SHELL * SHELL) ** -0.5, 0.375, ((0, 512),))
    owner_keys = jax.random.split(jax.random.fold_in(seeds[1], 1), TILES // TILES_DEV)
    owner_turns = jax.random.permutation(jax.random.fold_in(seeds[1], 3), TILES // TILES_DEV)
    owner = jax.vmap(lambda own, number: assign_block(jax.random.fold_in(seeds[1], 2), own, number, TILES_DEV, N_GX, 1, CAP, 2))(owner_keys, owner_turns).reshape((TILES, 1))
    quartet = draw_quartet(jax.random.fold_in(seeds[5], 71), 0)
    significance = touch_ends((jax.random.randint(seeds[3], (TILES,), 0, 4) < 3).astype(jnp.int32), jax.random.fold_in(seeds[3], 1), 0, 1)
    density = noise(seeds[4], (NBAS, NBAS), 1.0, 6.0, ((0, 16),))
    return dict(eri=eri, owner=owner, quartet=quartet, significance=significance, density=density)


def reference(eri, owner, quartet, significance, density):
    shell_count = NBAS // SHELL
    pair_size = SHELL * SHELL
    density_blocks = density.astype(jnp.float32).reshape(shell_count, SHELL, shell_count, SHELL)
    tile_index = jnp.arange(TILES, dtype=jnp.int32)
    device = tile_index // TILES_DEV
    z_index = device % N_GZ
    y_index = (device // N_GZ) % N_GY
    bra_shell = ((owner[:, 0] * N_GZ + z_index) * ROWSH + quartet[:, 0]).astype(jnp.int32)
    ket_shell = quartet[:, 1].astype(jnp.int32)
    row_shell = (y_index * DSLAB + quartet[:, 2]).astype(jnp.int32)
    col_shell = quartet[:, 3].astype(jnp.int32)
    blocks = density_blocks[row_shell, :, col_shell, :]
    weight = significance.astype(jnp.float32)
    groups = TILES // TILES_DEV

    def contract(operands):
        tile_data, flat_block, tile_weight = operands
        summed = jnp.einsum("tij,tj->ti", tile_data.astype(jnp.float32), flat_block)
        return summed * tile_weight[:, None]

    terms = lax.map(contract, (eri.reshape(groups, TILES_DEV, pair_size, pair_size),
                               blocks.reshape(groups, TILES_DEV, pair_size),
                               weight.reshape(groups, TILES_DEV)))
    terms = terms.reshape(TILES, SHELL, SHELL)
    result = jnp.zeros((shell_count, SHELL, shell_count, SHELL), jnp.float32)
    result = result.at[bra_shell, :, ket_shell, :].add(terms)
    return result.reshape(NBAS, NBAS)
```

```python
import jax
import jax.numpy as jnp
from jax import lax
from jax.experimental import pallas as pl
from jax.experimental.pallas import tpu as pltpu
from jax.sharding import PartitionSpec as P

SHELL = 16
PAIR = 256
TILES_DEV = 32
NSH = 192
N_GX = 8
N_Z = 8
N_GZ = 4
CAP = 8
ROWSH = 6
COLSH = 12
BLOCKS = ROWSH * COLSH
SLOTS = N_GX * CAP
CHUNKS = 8
MESH = pl.DeviceIdType.MESH
F32 = jnp.float32
BF16 = jnp.bfloat16
I32 = jnp.int32


def order(rel):
    return max(0, min(2 * rel - 1, 2 * (N_GX - rel)))


def iota(shape, dim):
    return lax.broadcasted_iota(I32, shape, dim)


def contract(own_s, quart_s, sig_s, dens_hbm, eri_hbm, val_ref, code_ref, dens, eri, picked, count_s, place_s, sems):
    per = TILES_DEV // CHUNKS
    dens_copy = pltpu.make_async_copy(dens_hbm, dens, sems.at[CHUNKS])
    dens_copy.start()
    copies = []
    for c in range(CHUNKS):
        part = pl.ds(c * per, per)
        copies.append(pltpu.make_async_copy(eri_hbm.at[part], eri.at[part], sems.at[c]))
        copies[-1].start()
    me = lax.axis_index("gx")
    val_ref[...] = jnp.zeros_like(val_ref)
    for i in range(N_GX):
        count_s[i] = 0
    lane = iota((1, 128), 1)
    codes = jnp.zeros((1, 128), I32)
    for t in range(TILES_DEV):
        rel = lax.rem(me - own_s[0, t] + N_GX, N_GX)
        row = jnp.maximum(0, jnp.minimum(2 * rel - 1, 2 * (N_GX - rel)))
        seen = count_s[row]
        count_s[row] = seen + 1
        place_s[t] = row * CAP + seen
        codes = jnp.where((lane & (SLOTS - 1)) == row * CAP + seen, quart_s[0, t] * NSH + quart_s[1, t], codes)
    for i in range(N_GX):
        code_ref[i] = jnp.where(((lane & (SLOTS - 1)) >> 3) == i, codes, 0)
    dens_copy.wait()
    group = iota((SHELL, 128), 1) >> 4
    for t in range(TILES_DEV):
        shell = quart_s[3, t]
        start = pl.multiple_of(quart_s[2, t] * SHELL, SHELL)
        column = pl.multiple_of((shell >> 3) * 128, 128)
        block = dens[pl.ds(start, SHELL), pl.ds(column, 128)].astype(F32)
        wanted = jnp.where(sig_s[0, t] != 0, shell & 7, -1)
        picked[t * SHELL:(t + 1) * SHELL, :] = jnp.where(group == wanted, block, 0.0)
    fold = ((iota((128, PAIR), 0) & 15) == (iota((128, PAIR), 1) & 15)).astype(F32).astype(BF16)
    wide = jnp.dot(picked[...].astype(BF16), fold, preferred_element_type=F32)
    rows = TILES_DEV * SHELL
    wide = jnp.where((iota((rows, PAIR), 0) & 15) == (iota((rows, PAIR), 1) >> 4), wide, 0.0).astype(BF16)
    gather = (iota((128, rows), 0) == (iota((128, rows), 1) >> 4)).astype(F32).astype(BF16)
    flat = jnp.dot(gather, wide, preferred_element_type=F32)
    weights = flat.T.astype(BF16)
    acc = jnp.zeros((PAIR, 128), F32)
    lanes = iota((PAIR, 128), 1)
    for c in range(CHUNKS):
        copies[c].wait()
        for t in range(c * per, (c + 1) * per):
            term = jnp.dot(eri[t], weights, preferred_element_type=F32)
            acc = jnp.where(lanes == t, term, acc)
    terms = acc.T
    for t in range(TILES_DEV):
        val_ref[pl.ds(place_s[t], 1), :] = terms[t:t + 1, :]


def exchange(val_ref, code_ref, out_ref, held, ycode, zcode, mine, half, arrived,
             ysend, yrecv, ycsend, ycrecv, zcsend, zcrecv, rsend, rrecv, psend, precv, xsend, xrecv):
    gx, gy, gz = lax.axis_index("gx"), lax.axis_index("gy"), lax.axis_index("gz")
    z, core = gy // 2, lax.rem(gy, 2)

    def along_x(d):
        return {"gx": lax.rem(gx + N_GX - d, N_GX)}

    def along_z(d):
        return {"gy": lax.rem(z + d + N_Z, N_Z) * 2 + core}

    def along_gz(d):
        return {"gz": lax.rem(gz + d, N_GZ)}

    partner = {"gy": z * 2 + 1 - core}
    barrier = pltpu.get_barrier_semaphore()
    peers = [along_x(d) for d in range(1, N_GX)] + [along_z(d) for d in range(1, N_Z)]
    peers += [along_gz(d) for d in range(1, N_GZ)] + [partner]
    for peer in peers:
        pl.semaphore_signal(barrier, inc=1, device_id=peer, device_id_type=MESH)
    pl.semaphore_wait(barrier, len(peers))

    def send(src, dst, s, r, peer):
        copy = pltpu.make_async_remote_copy(src_ref=src, dst_ref=dst, send_sem=s, recv_sem=r, device_id=peer, device_id_type=MESH)
        copy.start()
        return copy

    started = []
    near = [1, 7, 2]
    far = [6, 3, 5, 4]
    code_in, val_in = {}, {}
    for d in near + far:
        r = order(d)
        code_in[d] = send(code_ref.at[r], ycode.at[r], ycsend.at[r], ycrecv.at[r], along_x(d))
    for d in far[::-1] + near[::-1]:
        r = order(d)
        val_in[d] = send(val_ref.at[pl.ds(r * CAP, CAP)], held.at[0, pl.ds(r * CAP, CAP)], ysend.at[r], yrecv.at[r], along_x(d))
    held[0, 0:CAP, :] = val_ref[0:CAP, :]
    for d in near + far:
        code_in[d].wait_recv()
    total = code_ref[0]
    for r in range(1, N_GX):
        total = total + ycode[r]
    mine[...] = total
    zcode[0] = total
    zcode_in = []
    for d, slot in ((1, 1), (7, 2), (2, 3), (6, 4), (3, 5), (5, 6), (4, 7)):
        zcode_in.append(send(mine, zcode.at[slot], zcsend.at[slot], zcrecv.at[slot], along_z(d)))

    GR = SLOTS // 2

    def hop(src, direction, dst, g):
        part = pl.ds(g * GR, GR)
        i = (dst * 2 + g) if dst < 7 else (14 + g)
        c = send(held.at[src, part], held.at[dst, part], rsend.at[i], rrecv.at[i], along_z(direction))
        started.append(c)
        return c

    inward = {}
    for g, ds in ((0, near), (1, far)):
        for d in ds:
            val_in[d].wait_recv()
        inward[1, g] = hop(0, 1, 1, g)
        inward[2, g] = hop(0, -1, 2, g)

    rows = iota((2 * BLOCKS, 128), 0)
    other = (rows >= BLOCKS).astype(I32)
    inner = rows - other * BLOCKS
    bra = jnp.zeros_like(inner)
    for i in range(1, ROWSH):
        bra = bra + (inner >= i * COLSH).astype(I32)
    ket = inner - bra * COLSH
    column = jnp.where(other == 1, (z * 2 + 1 - core) * COLSH, gy * COLSH)
    wanted = bra * NSH + column + ket
    lane = iota((1, 128), 1)

    def place(a, b, acc):
        code = jnp.where(lane < SLOTS, zcode[a], zcode[b])
        hot = (wanted == code).astype(F32).astype(BF16)
        hot = jnp.concatenate([hot, hot], axis=1)
        values = jnp.concatenate([held[a], held[b]], axis=0)
        top = values.astype(BF16)
        low = (values - top.astype(F32)).astype(BF16)
        return acc + jnp.dot(hot, jnp.concatenate([top, low], axis=0), preferred_element_type=F32)

    acc = jnp.zeros((2 * BLOCKS, PAIR), F32)
    for c in zcode_in:
        c.wait_recv()
    for h in (1, 2, 3):
        left, right = 2 * h - 1, 2 * h
        for g in (0, 1):
            inward[left, g].wait_recv()
            if h < 3:
                inward[left + 2, g] = hop(left, 1, left + 2, g)
            elif g == 0:
                inward[7, 0] = hop(left, 1, 7, 0)
            inward[right, g].wait_recv()
            if h < 3:
                inward[right + 2, g] = hop(right, -1, right + 2, g)
            elif g == 1:
                inward[7, 1] = hop(right, -1, 7, 1)
        acc = place(left, right, acc)
    inward[7, 0].wait_recv()
    inward[7, 1].wait_recv()
    acc = place(0, 7, acc)
    half[...] = acc[BLOCKS:]
    give = send(half, arrived, psend, precv, partner)
    give.wait_recv()
    final = acc[:BLOCKS] + arrived[...]
    out_ref[0, gz] = final[:, :128]
    out_ref[1, gz] = final[:, 128:]
    last = []
    for d in range(1, N_GZ):
        last.append(send(out_ref.at[:, gz], out_ref.at[:, gz], xsend.at[d - 1], xrecv.at[d - 1], along_gz(d)))
    for c in last:
        c.wait_recv()
    for c in list(code_in.values()) + list(val_in.values()) + zcode_in + started + [give] + last:
        c.wait_send()


def assemble(got_ref, out_ref, wide):
    group = iota((4 * ROWSH, 128), 1) >> 4
    pieces = [[got_ref[pl.ds(h * N_GZ * BLOCKS + k, 4 * ROWSH, stride=COLSH), :] for h in range(2)] for k in range(COLSH)]
    for a in range(SHELL):
        for j, ks in enumerate((range(8), range(8, COLSH))):
            line = jnp.zeros((4 * ROWSH, 128), F32)
            for k in ks:
                shift = ((k - a) % 8) * 16
                src = pieces[k][a // 8]
                moved = pltpu.roll(src, shift, 1) if shift else src
                line = jnp.where(group == k % 8, moved, line)
            wide[j, pl.ds(a, 4 * ROWSH, stride=SHELL), :] = line
    out_ref[:128, :] = wide[0].T
    out_ref[128:, :] = wide[1].T[:NSH - 128, :]


def shards(eri, owner, quartet, significance, density):
    any_spec = pl.BlockSpec(memory_space=pl.ANY)
    smem = pl.BlockSpec(memory_space=pltpu.SMEM)
    vmem = pl.BlockSpec(memory_space=pltpu.VMEM)
    values, codes = pl.pallas_call(
        contract,
        out_shape=(jax.ShapeDtypeStruct((SLOTS, PAIR), F32), jax.ShapeDtypeStruct((N_GX, 1, 128), I32)),
        in_specs=[smem, smem, smem, any_spec, any_spec],
        out_specs=(vmem, vmem),
        scratch_shapes=[
            pltpu.VMEM(density.shape, BF16),
            pltpu.VMEM(eri.shape, BF16),
            pltpu.VMEM((TILES_DEV * SHELL, 128), F32),
            pltpu.SMEM((N_GX,), I32),
            pltpu.SMEM((TILES_DEV,), I32),
            pltpu.SemaphoreType.DMA((CHUNKS + 1,)),
        ],
        name="contract",
    )(owner.T, quartet.T, significance[None, :], density, eri)
    dma = pltpu.SemaphoreType.DMA
    got = pl.pallas_call(
        exchange,
        out_shape=jax.ShapeDtypeStruct((2, N_GZ, BLOCKS, 128), F32),
        in_specs=[vmem, vmem],
        out_specs=vmem,
        scratch_shapes=[
            pltpu.VMEM((N_Z, SLOTS, PAIR), F32),
            pltpu.VMEM((N_GX, 1, 128), I32),
            pltpu.VMEM((N_Z, 1, 128), I32),
            pltpu.VMEM((1, 128), I32),
            pltpu.VMEM((BLOCKS, PAIR), F32),
            pltpu.VMEM((BLOCKS, PAIR), F32),
            dma((N_GX,)), dma((N_GX,)), dma((N_GX,)), dma((N_GX,)), dma((N_Z,)), dma((N_Z,)),
            dma((16,)), dma((16,)), dma, dma, dma((N_GZ,)), dma((N_GZ,)),
        ],
        compiler_params=pltpu.CompilerParams(collective_id=0, has_side_effects=True),
        name="exchange",
    )(values, codes)
    turned = pl.pallas_call(
        assemble,
        out_shape=jax.ShapeDtypeStruct((NSH, N_GZ * ROWSH * SHELL), F32),
        in_specs=[vmem],
        out_specs=vmem,
        scratch_shapes=[pltpu.VMEM((2, N_GZ * ROWSH * SHELL, 128), F32)],
        name="assemble",
    )(got.reshape(2 * N_GZ * BLOCKS, 128))
    return turned.T


def solution(mesh):
    in_specs = (
        P(("gx", "gy", "gz"), None, None),
        P(("gx", "gy", "gz"), None),
        P(("gx", "gy", "gz"), None),
        P(("gx", "gy", "gz")),
        P("gy", None),
    )
    return jax.shard_map(shards, mesh=mesh, in_specs=in_specs, out_specs=P("gx", "gy"), check_vma=False)
```

```python
import jax
import jax.numpy as jnp
from jax import lax
from jax.experimental import pallas as pl
from jax.experimental.pallas import tpu as pltpu
from jax.sharding import PartitionSpec as P

SHELL = 16
PAIR = 256
TILES_DEV = 32
NSH = 192
N_GX = 8
N_Z = 8
N_GZ = 4
CAP = 8
ROWSH = 6
COLSH = 12
BLOCKS = ROWSH * COLSH
SLOTS = N_GX * CAP
CHUNKS = 8
DCHUNKS = 24
MESH = pl.DeviceIdType.MESH
F32 = jnp.float32
BF16 = jnp.bfloat16
I32 = jnp.int32


def order(rel):
    return max(0, min(2 * rel - 1, 2 * (N_GX - rel)))


def iota(shape, dim):
    return lax.broadcasted_iota(I32, shape, dim)


def fused(own_s, quart_s, sig_s, dens_hbm, eri_hbm, out_ref, dens, eri, picked, vals, codes_out, held, ycode, zcode, mine, hots, half, arrived,
          dsem, esem, ysend, yrecv, ycsend, ycrecv, zcsend, zcrecv, rsend, rrecv, psend, precv, xsend, xrecv):
    gx, gy, gz = lax.axis_index("gx"), lax.axis_index("gy"), lax.axis_index("gz")
    z, core = gy // 2, lax.rem(gy, 2)

    def along_x(d):
        return {"gx": lax.rem(gx + N_GX - d, N_GX)}

    def along_z(d):
        return {"gy": lax.rem(z + d + N_Z, N_Z) * 2 + core}

    def along_gz(d):
        return {"gz": lax.rem(gz + d + N_GZ, N_GZ)}

    partner = {"gy": z * 2 + 1 - core}
    loads = []
    for c in range(DCHUNKS):
        loads.append(pltpu.make_async_copy(dens_hbm.at[:, :, pl.ds(c * 128, 128)], dens.at[pl.ds(c * COLSH, COLSH)], dsem.at[c]))
        loads[-1].start()
    per = TILES_DEV // CHUNKS
    copies = []
    for c in range(CHUNKS):
        part = pl.ds(c * per, per)
        copies.append(pltpu.make_async_copy(eri_hbm.at[part], eri.at[part], esem.at[c]))
        copies[-1].start()
    barrier = pltpu.get_barrier_semaphore()
    peers = [along_x(d) for d in range(1, N_GX)] + [along_z(d) for d in range(1, N_Z)]
    peers += [along_gz(1), along_gz(-1), partner]
    for peer in peers:
        pl.semaphore_signal(barrier, inc=1, device_id=peer, device_id_type=MESH)

    rows = TILES_DEV * SHELL
    lane = iota((1, 128), 1)
    tile = iota((1, rows), 1) >> 4
    codes = jnp.zeros((1, 128), I32)
    spread = jnp.zeros((1, rows), I32)
    counts = jnp.int32(0)
    places = []
    for t in range(TILES_DEV):
        rel = (gx - own_s[0, t] + N_GX) & (N_GX - 1)
        row = jnp.maximum(0, jnp.minimum(2 * rel - 1, 2 * (N_GX - rel)))
        seen = (counts >> (row * 4)) & 15
        counts = counts + (jnp.int32(1) << (row * 4))
        slot = row * CAP + seen
        places.append(slot)
        codes = jnp.where((lane & (SLOTS - 1)) == slot, quart_s[0, t] * NSH + quart_s[1, t], codes)
        spread = jnp.where(tile == t, slot, spread)
    for i in range(N_GX):
        codes_out[i] = jnp.where(((lane & (SLOTS - 1)) >> 3) == i, codes, 0)
    gather = (iota((128, rows), 0) == spread).astype(F32).astype(BF16)
    fold = ((iota((128, PAIR), 0) & 15) == (iota((128, PAIR), 1) & 15)).astype(F32).astype(BF16)
    for load in loads:
        load.wait()
    group = iota((SHELL, 128), 1) >> 4
    for t in range(TILES_DEV):
        shell = quart_s[3, t]
        block = dens[(shell >> 3) * COLSH + quart_s[2, t]].astype(F32)
        wanted = jnp.where(sig_s[0, t] != 0, shell & 7, -1)
        picked[t * SHELL:(t + 1) * SHELL, :] = jnp.where(group == wanted, block, 0.0)
    wide = jnp.dot(picked[...].astype(BF16), fold, preferred_element_type=F32)
    wide = jnp.where((iota((rows, PAIR), 0) & 15) == (iota((rows, PAIR), 1) >> 4), wide, 0.0).astype(BF16)
    flat = jnp.dot(gather, wide, preferred_element_type=F32)
    weights = flat.T.astype(BF16)
    terms = jnp.zeros((PAIR, 128), F32)
    lanes = iota((PAIR, 128), 1)
    for c in range(CHUNKS):
        copies[c].wait()
        for t in range(c * per, (c + 1) * per):
            term = jnp.dot(eri[t], weights, preferred_element_type=F32)
            terms = jnp.where(lanes == places[t], term, terms)
    turned = terms.T
    vals[...] = turned[:SLOTS]
    held[0, 0:CAP, :] = turned[:CAP]

    pl.semaphore_wait(barrier, len(peers))

    def send(src, dst, s, r, peer):
        copy = pltpu.make_async_remote_copy(src_ref=src, dst_ref=dst, send_sem=s, recv_sem=r, device_id=peer, device_id_type=MESH)
        copy.start()
        return copy

    near = [1, 7, 2]
    far = [6, 3, 5, 4]
    code_in, val_in = {}, {}
    for d in far[::-1] + near[::-1]:
        r = order(d)
        code_in[d] = send(codes_out.at[r], ycode.at[r], ycsend.at[r], ycrecv.at[r], along_x(d))
        val_in[d] = send(vals.at[pl.ds(r * CAP, CAP)], held.at[0, pl.ds(r * CAP, CAP)], ysend.at[r], yrecv.at[r], along_x(d))

    started = []
    GR = SLOTS // 2

    def hop(src, distance, dst, g):
        part = pl.ds(g * GR, GR)
        i = dst * 2 + g
        c = send(held.at[src, part], held.at[dst, part], rsend.at[i], rrecv.at[i], along_z(distance))
        started.append(c)
        inward[dst, g] = c

    inward = {}
    rows = iota((2 * BLOCKS, 128), 0)
    other = (rows >= BLOCKS).astype(I32)
    inner = rows - other * BLOCKS
    bra = jnp.zeros_like(inner)
    for i in range(1, ROWSH):
        bra = bra + (inner >= i * COLSH).astype(I32)
    ket = inner - bra * COLSH
    column = jnp.where(other == 1, (z * 2 + 1 - core) * COLSH, gy * COLSH)
    wanted = bra * NSH + column + ket

    for g, ds in ((0, near), (1, far)):
        for d in ds:
            val_in[d].wait_recv()
        hop(0, 2, 3, g)
        hop(0, -2, 4, g)
        hop(0, 1, 1, g)
        hop(0, -1, 2, g)
    for d in near + far:
        code_in[d].wait_recv()
    total = codes_out[0]
    for r in range(1, N_GX):
        total = total + ycode[r]
    mine[...] = total
    zcode[0] = total
    zcode_in = []
    for d, slot in ((4, 7), (3, 5), (5, 6), (2, 3), (6, 4), (1, 1), (7, 2)):
        zcode_in.append(send(mine, zcode.at[slot], zcsend.at[slot], zcrecv.at[slot], along_z(d)))

    inward[3, 0].wait_recv()
    hop(3, 2, 7, 0)
    hop(3, 1, 5, 0)
    inward[4, 0].wait_recv()
    hop(4, -1, 6, 0)
    inward[4, 1].wait_recv()
    hop(4, -2, 7, 1)
    hop(4, -1, 6, 1)
    inward[3, 1].wait_recv()
    hop(3, 1, 5, 1)

    for c in zcode_in:
        c.wait_recv()
    pairs = [(1, 2), (3, 4), (5, 6), (0, 7)]
    for i, (a, b) in enumerate(pairs):
        code = jnp.where(lane < SLOTS, zcode[a], zcode[b])
        hot = (wanted == code).astype(F32).astype(BF16)
        hots[i, :, 0:128] = hot
        hots[i, :, 128:256] = hot

    acc = jnp.zeros((2 * BLOCKS, PAIR), F32)
    for i, (a, b) in enumerate(pairs):
        for s in (a, b):
            if s not in (0, 3, 4):
                inward[s, 0].wait_recv()
                inward[s, 1].wait_recv()
        values = jnp.concatenate([held[a], held[b]], axis=0)
        top = values.astype(BF16)
        low = (values - top.astype(F32)).astype(BF16)
        acc = acc + jnp.dot(hots[i], jnp.concatenate([top, low], axis=0), preferred_element_type=F32)
    half[...] = acc[BLOCKS:]
    give = send(half, arrived, psend, precv, partner)
    give.wait_recv()
    final = acc[:BLOCKS] + arrived[...]
    out_ref[0, gz] = final[:, :128]
    out_ref[1, gz] = final[:, 128:]

    def pass_on(h, owner, i, direction):
        part = out_ref.at[h, owner]
        c = send(part, part, xsend.at[i], xrecv.at[i], along_gz(direction))
        started.append(c)
        return c

    prev, nxt = lax.rem(gz + N_GZ - 1, N_GZ), lax.rem(gz + 1, N_GZ)
    up0 = pass_on(0, gz, 0, 1)
    down1 = pass_on(1, gz, 1, -1)
    up1 = pass_on(1, gz, 2, 1)
    down0 = pass_on(0, gz, 3, -1)
    up0.wait_recv()
    two0 = pass_on(0, prev, 4, 1)
    down1.wait_recv()
    two1 = pass_on(1, nxt, 5, -1)
    for c in (up1, down0, two0, two1):
        c.wait_recv()
    for c in list(code_in.values()) + list(val_in.values()) + zcode_in + started + [give]:
        c.wait_send()


def assemble(got_ref, out_ref, wide):
    group = iota((4 * ROWSH, 128), 1) >> 4
    pieces = [[got_ref[pl.ds(h * N_GZ * BLOCKS + k, 4 * ROWSH, stride=COLSH), :] for h in range(2)] for k in range(COLSH)]
    for a in range(SHELL):
        for j, ks in enumerate((range(8), range(8, COLSH))):
            line = jnp.zeros((4 * ROWSH, 128), F32)
            for k in ks:
                shift = ((k - a) % 8) * 16
                src = pieces[k][a // 8]
                moved = pltpu.roll(src, shift, 1) if shift else src
                line = jnp.where(group == k % 8, moved, line)
            wide[j, pl.ds(a, 4 * ROWSH, stride=SHELL), :] = line
    out_ref[:128, :] = wide[0].T
    out_ref[128:, :] = wide[1].T[:NSH - 128, :]


def shards(eri, owner, quartet, significance, density):
    hbm = pl.BlockSpec(memory_space=pltpu.HBM)
    smem = pl.BlockSpec(memory_space=pltpu.SMEM)
    vmem = pl.BlockSpec(memory_space=pltpu.VMEM)
    dma = pltpu.SemaphoreType.DMA
    got = pl.pallas_call(
        fused,
        out_shape=jax.ShapeDtypeStruct((2, N_GZ, BLOCKS, 128), F32),
        in_specs=[smem, smem, smem, hbm, hbm],
        out_specs=vmem,
        scratch_shapes=[
            pltpu.VMEM((DCHUNKS * COLSH, SHELL, 128), BF16),
            pltpu.VMEM(eri.shape, BF16),
            pltpu.VMEM((TILES_DEV * SHELL, 128), F32),
            pltpu.VMEM((SLOTS, PAIR), F32),
            pltpu.VMEM((N_GX, 1, 128), I32),
            pltpu.VMEM((N_Z, SLOTS, PAIR), F32),
            pltpu.VMEM((N_GX, 1, 128), I32),
            pltpu.VMEM((N_Z, 1, 128), I32),
            pltpu.VMEM((1, 128), I32),
            pltpu.VMEM((4, 2 * BLOCKS, PAIR), BF16),
            pltpu.VMEM((BLOCKS, PAIR), F32),
            pltpu.VMEM((BLOCKS, PAIR), F32),
            dma((DCHUNKS,)), dma((CHUNKS,)),
            dma((N_GX,)), dma((N_GX,)), dma((N_GX,)), dma((N_GX,)), dma((N_Z,)), dma((N_Z,)),
            dma((16,)), dma((16,)), dma, dma, dma((6,)), dma((6,)),
        ],
        compiler_params=pltpu.CompilerParams(collective_id=0, has_side_effects=True, vmem_limit_bytes=66600000),
        name="fused",
    )(owner.T, quartet.T, significance[None, :], density.reshape(COLSH, SHELL, density.shape[1]), eri)
    turned = pl.pallas_call(
        assemble,
        out_shape=jax.ShapeDtypeStruct((NSH, N_GZ * ROWSH * SHELL), F32),
        in_specs=[vmem],
        out_specs=vmem,
        scratch_shapes=[pltpu.VMEM((2, N_GZ * ROWSH * SHELL, 128), F32)],
        compiler_params=pltpu.CompilerParams(vmem_limit_bytes=66600000),
        name="assemble",
    )(got.reshape(2 * N_GZ * BLOCKS, 128))
    return turned.T


def solution(mesh):
    in_specs = (
        P(("gx", "gy", "gz"), None, None),
        P(("gx", "gy", "gz"), None),
        P(("gx", "gy", "gz"), None),
        P(("gx", "gy", "gz")),
        P("gy", None),
    )
    return jax.shard_map(shards, mesh=mesh, in_specs=in_specs, out_specs=P("gx", "gy"), check_vma=False)
```

```python
import jax
import jax.numpy as jnp
from jax import lax
from jax.experimental import pallas as pl
from jax.experimental.pallas import tpu as pltpu
from jax.sharding import PartitionSpec as P

SHELL = 16
PAIR = 256
TILES_DEV = 32
NSH = 192
N_GX = 8
N_Z = 8
N_GZ = 4
CAP = 8
ROWSH = 6
COLSH = 12
BLOCKS = ROWSH * COLSH
SLOTS = N_GX * CAP
CHUNKS = 8
DCHUNKS = 24
MESH = pl.DeviceIdType.MESH
F32 = jnp.float32
BF16 = jnp.bfloat16
I32 = jnp.int32


def order(rel):
    return max(0, min(2 * rel - 1, 2 * (N_GX - rel)))


def iota(shape, dim):
    return lax.broadcasted_iota(I32, shape, dim)


def fused(own_h, quart_h, sig_h, dens_hbm, eri_hbm, out_ref, own_s, quart_s, sig_s, isem, dens, eri, picked, vals, codes_out, held, ycode, zcode, mine, hots, half, arrived,
          dsem, esem, ysend, yrecv, ycsend, ycrecv, zcsend, zcrecv, rsend, rrecv, psend, precv, xsend, xrecv):
    gx, gy, gz = lax.axis_index("gx"), lax.axis_index("gy"), lax.axis_index("gz")
    z, core = gy // 2, lax.rem(gy, 2)

    def along_x(d):
        return {"gx": lax.rem(gx + N_GX - d, N_GX)}

    def along_z(d):
        return {"gy": lax.rem(z + d + N_Z, N_Z) * 2 + core}

    def along_gz(d):
        return {"gz": lax.rem(gz + d + N_GZ, N_GZ)}

    partner = {"gy": z * 2 + 1 - core}
    ints = []
    for i, (src, dst) in enumerate(((own_h, own_s), (quart_h, quart_s), (sig_h, sig_s))):
        ints.append(pltpu.make_async_copy(src, dst, isem.at[i]))
        ints[-1].start()
    loads = []
    for c in range(DCHUNKS):
        loads.append(pltpu.make_async_copy(dens_hbm.at[:, :, pl.ds(c * 128, 128)], dens.at[pl.ds(c * COLSH, COLSH)], dsem.at[c]))
        loads[-1].start()
    per = TILES_DEV // CHUNKS
    copies = []
    for c in range(CHUNKS):
        part = pl.ds(c * per, per)
        copies.append(pltpu.make_async_copy(eri_hbm.at[part], eri.at[part], esem.at[c]))
        copies[-1].start()
    barrier = pltpu.get_barrier_semaphore()
    peers = [along_x(d) for d in range(1, N_GX)] + [along_z(d) for d in range(1, N_Z)]
    peers += [along_gz(1), along_gz(-1), partner]
    for peer in peers:
        pl.semaphore_signal(barrier, inc=1, device_id=peer, device_id_type=MESH)

    rows = TILES_DEV * SHELL
    lane = iota((1, 128), 1)
    tile = iota((1, rows), 1) >> 4
    codes = jnp.zeros((1, 128), I32)
    spread = jnp.zeros((1, rows), I32)
    counts = jnp.int32(0)
    places = []
    for c in ints:
        c.wait()
    for t in range(TILES_DEV):
        rel = (gx - own_s[0, t] + N_GX) & (N_GX - 1)
        row = jnp.maximum(0, jnp.minimum(2 * rel - 1, 2 * (N_GX - rel)))
        seen = (counts >> (row * 4)) & 15
        counts = counts + (jnp.int32(1) << (row * 4))
        slot = row * CAP + seen
        places.append(slot)
        codes = jnp.where((lane & (SLOTS - 1)) == slot, quart_s[0, t] * NSH + quart_s[1, t], codes)
        spread = jnp.where(tile == t, slot, spread)
    for i in range(N_GX):
        codes_out[i] = jnp.where(((lane & (SLOTS - 1)) >> 3) == i, codes, 0)
    gather = (iota((128, rows), 0) == spread).astype(F32).astype(BF16)
    fold = ((iota((128, PAIR), 0) & 15) == (iota((128, PAIR), 1) & 15)).astype(F32).astype(BF16)
    for load in loads:
        load.wait()
    group = iota((SHELL, 128), 1) >> 4
    for t in range(TILES_DEV):
        shell = quart_s[3, t]
        block = dens[(shell >> 3) * COLSH + quart_s[2, t]].astype(F32)
        wanted = jnp.where(sig_s[0, t] != 0, shell & 7, -1)
        picked[t * SHELL:(t + 1) * SHELL, :] = jnp.where(group == wanted, block, 0.0)
    wide = jnp.dot(picked[...].astype(BF16), fold, preferred_element_type=F32)
    wide = jnp.where((iota((rows, PAIR), 0) & 15) == (iota((rows, PAIR), 1) >> 4), wide, 0.0).astype(BF16)
    flat = jnp.dot(gather, wide, preferred_element_type=F32)
    weights = flat[:SLOTS].astype(BF16)
    terms = jnp.zeros((SLOTS, PAIR), F32)
    slots = iota((SLOTS, PAIR), 0)
    for c in copies:
        c.wait()
    step = 4
    for t in range(0, TILES_DEV, step):
        many = lax.dot_general(weights, eri[t:t + step].reshape(step * PAIR, PAIR), (((1,), (1,)), ((), ())), preferred_element_type=F32)
        for i in range(step):
            terms = jnp.where(slots == places[t + i], many[:, i * PAIR:(i + 1) * PAIR], terms)
    vals[...] = terms
    held[0, 0:CAP, :] = terms[:CAP]

    pl.semaphore_wait(barrier, len(peers))

    def send(src, dst, s, r, peer):
        copy = pltpu.make_async_remote_copy(src_ref=src, dst_ref=dst, send_sem=s, recv_sem=r, device_id=peer, device_id_type=MESH)
        copy.start()
        return copy

    near = [1, 7, 2]
    far = [6, 3, 5, 4]
    code_in, val_in = {}, {}
    for d in far[::-1] + near[::-1]:
        r = order(d)
        code_in[d] = send(codes_out.at[r], ycode.at[r], ycsend.at[r], ycrecv.at[r], along_x(d))
        val_in[d] = send(vals.at[pl.ds(r * CAP, CAP)], held.at[0, pl.ds(r * CAP, CAP)], ysend.at[r], yrecv.at[r], along_x(d))

    started = []
    GR = SLOTS // 2

    def hop(src, distance, dst, g):
        part = pl.ds(g * GR, GR)
        i = dst * 2 + g
        c = send(held.at[src, part], held.at[dst, part], rsend.at[i], rrecv.at[i], along_z(distance))
        started.append(c)
        inward[dst, g] = c

    inward = {}
    rows = iota((2 * BLOCKS, 128), 0)
    other = (rows >= BLOCKS).astype(I32)
    inner = rows - other * BLOCKS
    bra = jnp.zeros_like(inner)
    for i in range(1, ROWSH):
        bra = bra + (inner >= i * COLSH).astype(I32)
    ket = inner - bra * COLSH
    column = jnp.where(other == 1, (z * 2 + 1 - core) * COLSH, gy * COLSH)
    wanted = bra * NSH + column + ket

    for g, ds in ((0, near), (1, far)):
        for d in ds:
            val_in[d].wait_recv()
        hop(0, 2, 3, g)
        hop(0, -2, 4, g)
        hop(0, 1, 1, g)
        hop(0, -1, 2, g)
    for d in near + far:
        code_in[d].wait_recv()
    total = codes_out[0]
    for r in range(1, N_GX):
        total = total + ycode[r]
    mine[...] = total
    zcode[0] = total
    zcode_in = []
    for d, slot in ((4, 7), (3, 5), (5, 6), (2, 3), (6, 4), (1, 1), (7, 2)):
        zcode_in.append(send(mine, zcode.at[slot], zcsend.at[slot], zcrecv.at[slot], along_z(d)))

    inward[3, 0].wait_recv()
    hop(3, 2, 7, 0)
    hop(3, 1, 5, 0)
    inward[4, 0].wait_recv()
    hop(4, -1, 6, 0)
    inward[4, 1].wait_recv()
    hop(4, -2, 7, 1)
    hop(4, -1, 6, 1)
    inward[3, 1].wait_recv()
    hop(3, 1, 5, 1)

    for c in zcode_in:
        c.wait_recv()
    pairs = [(1, 2), (3, 4), (5, 6), (0, 7)]
    for i, (a, b) in enumerate(pairs):
        code = jnp.where(lane < SLOTS, zcode[a], zcode[b])
        hot = (wanted == code).astype(F32).astype(BF16)
        hots[i, :, 0:128] = hot
        hots[i, :, 128:256] = hot

    acc = jnp.zeros((2 * BLOCKS, PAIR), F32)
    for i, (a, b) in enumerate(pairs):
        for s in (a, b):
            if s not in (0, 3, 4):
                inward[s, 0].wait_recv()
                inward[s, 1].wait_recv()
        values = jnp.concatenate([held[a], held[b]], axis=0)
        top = values.astype(BF16)
        low = (values - top.astype(F32)).astype(BF16)
        acc = acc + jnp.dot(hots[i], jnp.concatenate([top, low], axis=0), preferred_element_type=F32)
    half[...] = acc[BLOCKS:]
    give = send(half, arrived, psend, precv, partner)
    give.wait_recv()
    final = acc[:BLOCKS] + arrived[...]
    out_ref[0, gz] = final[:, :128]
    out_ref[1, gz] = final[:, 128:]

    def pass_on(h, owner, i, direction):
        part = out_ref.at[h, owner]
        c = send(part, part, xsend.at[i], xrecv.at[i], along_gz(direction))
        started.append(c)
        return c

    prev, nxt = lax.rem(gz + N_GZ - 1, N_GZ), lax.rem(gz + 1, N_GZ)
    up0 = pass_on(0, gz, 0, 1)
    down1 = pass_on(1, gz, 1, -1)
    up1 = pass_on(1, gz, 2, 1)
    down0 = pass_on(0, gz, 3, -1)
    up0.wait_recv()
    two0 = pass_on(0, prev, 4, 1)
    down1.wait_recv()
    two1 = pass_on(1, nxt, 5, -1)
    for c in (up1, down0, two0, two1):
        c.wait_recv()
    for c in list(code_in.values()) + list(val_in.values()) + zcode_in + started + [give]:
        c.wait_send()


def assemble(got_ref, out_ref, wide):
    group = iota((4 * ROWSH, 128), 1) >> 4
    pieces = [[got_ref[pl.ds(h * N_GZ * BLOCKS + k, 4 * ROWSH, stride=COLSH), :] for h in range(2)] for k in range(COLSH)]
    for a in range(SHELL):
        for j, ks in enumerate((range(8), range(8, COLSH))):
            line = jnp.zeros((4 * ROWSH, 128), F32)
            for k in ks:
                shift = ((k - a) % 8) * 16
                src = pieces[k][a // 8]
                moved = pltpu.roll(src, shift, 1) if shift else src
                line = jnp.where(group == k % 8, moved, line)
            wide[j, pl.ds(a, 4 * ROWSH, stride=SHELL), :] = line
    out_ref[:128, :] = wide[0].T
    out_ref[128:, :] = wide[1].T[:NSH - 128, :]


def shards(eri, owner, quartet, significance, density):
    hbm = pl.BlockSpec(memory_space=pltpu.HBM)
    vmem = pl.BlockSpec(memory_space=pltpu.VMEM)
    dma = pltpu.SemaphoreType.DMA
    operands = (owner.T, quartet.T, significance[None, :], density.reshape(COLSH, SHELL, density.shape[1]), eri)
    got = pl.pallas_call(
        fused,
        out_shape=jax.ShapeDtypeStruct((2, N_GZ, BLOCKS, 128), F32),
        in_specs=[hbm] * 5,
        out_specs=vmem,
        scratch_shapes=[
            pltpu.SMEM((1, TILES_DEV), I32),
            pltpu.SMEM((4, TILES_DEV), I32),
            pltpu.SMEM((1, TILES_DEV), I32),
            dma((3,)),
            pltpu.VMEM((DCHUNKS * COLSH, SHELL, 128), BF16),
            pltpu.VMEM(eri.shape, BF16),
            pltpu.VMEM((TILES_DEV * SHELL, 128), F32),
            pltpu.VMEM((SLOTS, PAIR), F32),
            pltpu.VMEM((N_GX, 1, 128), I32),
            pltpu.VMEM((N_Z, SLOTS, PAIR), F32),
            pltpu.VMEM((N_GX, 1, 128), I32),
            pltpu.VMEM((N_Z, 1, 128), I32),
            pltpu.VMEM((1, 128), I32),
            pltpu.VMEM((4, 2 * BLOCKS, PAIR), BF16),
            pltpu.VMEM((BLOCKS, PAIR), F32),
            pltpu.VMEM((BLOCKS, PAIR), F32),
            dma((DCHUNKS,)), dma((CHUNKS,)),
            dma((N_GX,)), dma((N_GX,)), dma((N_GX,)), dma((N_GX,)), dma((N_Z,)), dma((N_Z,)),
            dma((16,)), dma((16,)), dma, dma, dma((6,)), dma((6,)),
        ],
        compiler_params=pltpu.CompilerParams(collective_id=0, has_side_effects=True, vmem_limit_bytes=16000000),
        name="fused",
    )(*[pltpu.with_memory_space_constraint(a, pltpu.HBM) for a in operands])
    turned = pl.pallas_call(
        assemble,
        out_shape=jax.ShapeDtypeStruct((NSH, N_GZ * ROWSH * SHELL), F32),
        in_specs=[vmem],
        out_specs=vmem,
        scratch_shapes=[pltpu.VMEM((2, N_GZ * ROWSH * SHELL, 128), F32)],
        compiler_params=pltpu.CompilerParams(vmem_limit_bytes=16000000),
        name="assemble",
    )(got.reshape(2 * N_GZ * BLOCKS, 128))
    return turned.T


def solution(mesh):
    in_specs = (
        P(("gx", "gy", "gz"), None, None),
        P(("gx", "gy", "gz"), None),
        P(("gx", "gy", "gz"), None),
        P(("gx", "gy", "gz")),
        P("gy", None),
    )
    return jax.shard_map(shards, mesh=mesh, in_specs=in_specs, out_specs=P("gx", "gy"), check_vma=False)
```

```python
import jax
import jax.numpy as jnp
from jax import lax
from jax.experimental import pallas as pl
from jax.experimental.pallas import tpu as pltpu
from jax.sharding import PartitionSpec as P

SHELL = 16
PAIR = 256
TILES_DEV = 32
NSH = 192
N_GX = 8
N_Z = 8
N_GZ = 4
CAP = 8
ROWSH = 6
COLSH = 12
BLOCKS = ROWSH * COLSH
SLOTS = N_GX * CAP
CHUNKS = 2
DCHUNKS = 24
MESH = pl.DeviceIdType.MESH
F32 = jnp.float32
BF16 = jnp.bfloat16
I32 = jnp.int32


def order(rel):
    return max(0, min(2 * rel - 1, 2 * (N_GX - rel)))


def iota(shape, dim):
    return lax.broadcasted_iota(I32, shape, dim)


def fused(own_h, quart_h, sig_h, dens_hbm, eri_hbm, out_ref, own_s, quart_s, sig_s, isem, dens, eri, picked, vals, codes_out, held, ycode, zcode, mine, hots, half,
          dsem, esem, ysend, yrecv, ycsend, ycrecv, zcsend, zcrecv, rsend, rrecv, xsend, xrecv):
    gx, gy, gz = lax.axis_index("gx"), lax.axis_index("gy"), lax.axis_index("gz")
    z, core = gy // 2, lax.rem(gy, 2)

    def along_x(d, c):
        return {"gx": lax.rem(gx + N_GX - d, N_GX), "gy": z * 2 + c}

    def along_z(d):
        return {"gy": lax.rem(z + d + N_Z, N_Z) * 2 + core}

    def along_gz(d, c):
        return {"gy": z * 2 + c, "gz": lax.rem(gz + d + N_GZ, N_GZ)}

    mate = 1 - core
    step = 1 - 2 * core
    partner = {"gy": z * 2 + mate}
    ints = []
    for i, (src, dst) in enumerate(((own_h, own_s), (quart_h, quart_s), (sig_h, sig_s))):
        ints.append(pltpu.make_async_copy(src, dst, isem.at[i]))
        ints[-1].start()
    loads = []
    for c in range(DCHUNKS):
        loads.append(pltpu.make_async_copy(dens_hbm.at[:, :, pl.ds(c * 128, 128)], dens.at[pl.ds(c * COLSH, COLSH)], dsem.at[c]))
        loads[-1].start()
    per = TILES_DEV // CHUNKS
    copies = []
    for c in range(CHUNKS):
        part = pl.ds(c * per, per)
        copies.append(pltpu.make_async_copy(eri_hbm.at[part], eri.at[part], esem.at[c]))
        copies[-1].start()
    barrier = pltpu.get_barrier_semaphore()
    peers = [along_x(d, c) for d in range(1, N_GX) for c in range(2)] + [along_z(d) for d in range(1, N_Z)]
    peers += [along_gz(d, c) for d in (1, 2, 3) for c in range(2)] + [partner]
    for peer in peers:
        pl.semaphore_signal(barrier, inc=1, device_id=peer, device_id_type=MESH)

    rows = TILES_DEV * SHELL
    lane = iota((1, 128), 1)
    tile = iota((1, rows), 1) >> 4
    codes = jnp.zeros((1, 128), I32)
    spread = jnp.zeros((1, rows), I32)
    counts = jnp.int32(0)
    places = []
    for c in ints:
        c.wait()
    for t in range(TILES_DEV):
        rel = (gx - own_s[0, t] + N_GX) & (N_GX - 1)
        row = jnp.maximum(0, jnp.minimum(2 * rel - 1, 2 * (N_GX - rel)))
        seen = (counts >> (row * 4)) & 15
        counts = counts + (jnp.int32(1) << (row * 4))
        slot = row * CAP + seen
        places.append(slot)
        codes = jnp.where(lane == row * 2 * CAP + core * CAP + seen, quart_s[0, t] * NSH + quart_s[1, t], codes)
        spread = jnp.where(tile == t, slot, spread)
    for i in range(N_GX):
        codes_out[i] = jnp.where((lane >> 4) == i, codes, 0)
    gather = (iota((128, rows), 0) == spread).astype(F32).astype(BF16)
    fold = ((iota((128, PAIR), 0) & 15) == (iota((128, PAIR), 1) & 15)).astype(F32).astype(BF16)
    for load in loads:
        load.wait()
    group = iota((SHELL, 128), 1) >> 4
    for t in range(TILES_DEV):
        shell = quart_s[3, t]
        block = dens[(shell >> 3) * COLSH + quart_s[2, t]].astype(F32)
        wanted = jnp.where(sig_s[0, t] != 0, shell & 7, -1)
        picked[t * SHELL:(t + 1) * SHELL, :] = jnp.where(group == wanted, block, 0.0)
    wide = jnp.dot(picked[...].astype(BF16), fold, preferred_element_type=F32)
    wide = jnp.where((iota((rows, PAIR), 0) & 15) == (iota((rows, PAIR), 1) >> 4), wide, 0.0).astype(BF16)
    flat = jnp.dot(gather, wide, preferred_element_type=F32)
    weights = flat[:SLOTS].astype(BF16)
    terms = jnp.zeros((SLOTS, PAIR), F32)
    slots = iota((SLOTS, PAIR), 0)
    group = 4
    for t in range(0, TILES_DEV, group):
        if t % per == 0:
            copies[t // per].wait()
        many = lax.dot_general(weights, eri[t:t + group].reshape(group * PAIR, PAIR), (((1,), (1,)), ((), ())), preferred_element_type=F32)
        for i in range(group):
            terms = jnp.where(slots == places[t + i], many[:, i * PAIR:(i + 1) * PAIR], terms)
    vals[0] = terms[:, :128]
    vals[1] = terms[:, 128:]
    held[0, pl.ds(pl.multiple_of(core * CAP, CAP), CAP), :] = jnp.where(core == 0, terms[:CAP, :128], terms[:CAP, 128:])

    pl.semaphore_wait(barrier, len(peers))

    def link(src, dst, s, r, peer):
        return pltpu.make_async_remote_copy(src_ref=src, dst_ref=dst, send_sem=s, recv_sem=r, device_id=peer, device_id_type=MESH)

    def send(src, dst, s, r, peer):
        copy = link(src, dst, s, r, peer)
        copy.start()
        started.append(copy)
        return copy

    started = []
    near = [1, 7, 2]
    far = [6, 3, 5, 4]

    def value_rows(r, c):
        return held.at[0, pl.ds(pl.multiple_of(r * 2 * CAP + c * CAP, CAP), CAP)]

    def give(r, c, peer):
        send(codes_out.at[r], ycode.at[r * 2 + core], ycsend.at[r * 2 + c], ycrecv.at[r * 2 + core], peer)
        send(vals.at[c, pl.ds(r * CAP, CAP)], value_rows(r, core), ysend.at[r * 2 + c], yrecv.at[r * 2 + core], peer)

    for d in far[::-1] + near[::-1]:
        for c in range(2):
            give(order(d), c, along_x(d, c))
    give(0, mate, partner)

    def value_in(r, c):
        link(vals.at[0, pl.ds(0, CAP)], value_rows(r, c), ysend.at[0], yrecv.at[r * 2 + c], partner).wait_recv()

    def code_in(r, c):
        link(codes_out.at[0], ycode.at[r * 2 + c], ycsend.at[0], ycrecv.at[r * 2 + c], partner).wait_recv()

    firsts, sizes = (0, 64), (64, 64)

    def hop(src, distance, dst, g):
        part = pl.ds(firsts[g], sizes[g])
        i = dst * 2 + g
        inward[dst, g] = send(held.at[src, part], held.at[dst, part], rsend.at[i], rrecv.at[i], along_z(distance))

    inward = {}
    rows = iota((2 * BLOCKS, 128), 0)
    other = (rows >= BLOCKS).astype(I32)
    inner = rows - other * BLOCKS
    bra = jnp.zeros_like(inner)
    for i in range(1, ROWSH):
        bra = bra + (inner >= i * COLSH).astype(I32)
    ket = inner - bra * COLSH
    column = jnp.where(other == 1, (z * 2 + 1 - core) * COLSH, gy * COLSH)
    wanted = bra * NSH + column + ket

    value_in(0, mate)
    for g, ds in enumerate(((1, 7, 2), (6, 3, 5, 4))):
        for d in ds:
            for c in range(2):
                value_in(order(d), c)
        hop(0, 2, 3, g)
        hop(0, -2, 4, g)
        hop(0, 1, 1, g)
        hop(0, -1, 2, g)
    code_in(0, mate)
    total = codes_out[0] + ycode[mate]
    for r in range(1, N_GX):
        for c in range(2):
            code_in(r, c)
            total = total + ycode[r * 2 + c]
    mine[...] = total
    zcode[0] = total
    zcode_in = []
    for d, slot in ((4, 7), (3, 5), (5, 6), (2, 3), (6, 4), (1, 1), (7, 2)):
        zcode_in.append(send(mine, zcode.at[slot], zcsend.at[slot], zcrecv.at[slot], along_z(d)))

    for g in range(2):
        inward[3, g].wait_recv()
        if g in (0,):
            hop(3, 2, 7, g)
        hop(3, 1, 5, g)
        inward[4, g].wait_recv()
        if g not in (0,):
            hop(4, -2, 7, g)
        hop(4, -1, 6, g)

    for c in zcode_in:
        c.wait_recv()
    for i in range(N_Z):
        hot = (wanted == zcode[i]).astype(F32).astype(BF16)
        hots[i, :, 0:128] = hot
        hots[i, :, 128:256] = hot

    acc = jnp.zeros((2 * BLOCKS, 128), F32)
    for i in (0, 3, 4, 1, 2, 5, 6, 7):
        if i not in (0, 3, 4):
            for g in range(2):
                inward[i, g].wait_recv()
        top = held[i].astype(BF16)
        low = (held[i] - top.astype(F32)).astype(BF16)
        acc = acc + jnp.dot(hots[i], jnp.concatenate([top, low], axis=0), preferred_element_type=F32)
    half[...] = acc[BLOCKS:]
    out_ref[core, gz] = acc[:BLOCKS]

    home = out_ref.at[core, gz]

    def spread_out(i, src, peer):
        return send(src, home, xsend.at[i], xrecv.at[i], peer)

    last = [
        spread_out(6, half, partner),
        spread_out(4, home, along_gz(2, core)),
        spread_out(5, half, along_gz(2, mate)),
        spread_out(0, home, along_gz(step, core)),
        spread_out(1, half, along_gz(-step, mate)),
        spread_out(2, home, along_gz(-step, core)),
        spread_out(3, half, along_gz(step, mate)),
    ]
    for c in last:
        c.wait_recv()
    for c in started:
        c.wait_send()


def assemble(got_ref, out_ref, wide):
    group = iota((4 * ROWSH, 128), 1) >> 4
    pieces = [[got_ref[pl.ds(h * N_GZ * BLOCKS + k, 4 * ROWSH, stride=COLSH), :] for h in range(2)] for k in range(COLSH)]
    for a in range(SHELL):
        for j, ks in enumerate((range(8), range(8, COLSH))):
            line = jnp.zeros((4 * ROWSH, 128), F32)
            for k in ks:
                shift = ((k - a) % 8) * 16
                src = pieces[k][a // 8]
                moved = pltpu.roll(src, shift, 1) if shift else src
                line = jnp.where(group == k % 8, moved, line)
            wide[j, pl.ds(a, 4 * ROWSH, stride=SHELL), :] = line
    out_ref[:128, :] = wide[0].T
    out_ref[128:, :] = wide[1].T[:NSH - 128, :]


def shards(eri, owner, quartet, significance, density):
    hbm = pl.BlockSpec(memory_space=pltpu.HBM)
    vmem = pl.BlockSpec(memory_space=pltpu.VMEM)
    dma = pltpu.SemaphoreType.DMA
    operands = (owner.T, quartet.T, significance[None, :], density.reshape(COLSH, SHELL, density.shape[1]), eri)
    got = pl.pallas_call(
        fused,
        out_shape=jax.ShapeDtypeStruct((2, N_GZ, BLOCKS, 128), F32),
        in_specs=[hbm] * 5,
        out_specs=vmem,
        scratch_shapes=[
            pltpu.SMEM((1, TILES_DEV), I32),
            pltpu.SMEM((4, TILES_DEV), I32),
            pltpu.SMEM((1, TILES_DEV), I32),
            dma((3,)),
            pltpu.VMEM((DCHUNKS * COLSH, SHELL, 128), BF16),
            pltpu.VMEM(eri.shape, BF16),
            pltpu.VMEM((TILES_DEV * SHELL, 128), F32),
            pltpu.VMEM((2, SLOTS, 128), F32),
            pltpu.VMEM((N_GX, 1, 128), I32),
            pltpu.VMEM((N_Z, 2 * SLOTS, 128), F32),
            pltpu.VMEM((2 * N_GX, 1, 128), I32),
            pltpu.VMEM((N_Z, 1, 128), I32),
            pltpu.VMEM((1, 128), I32),
            pltpu.VMEM((N_Z, 2 * BLOCKS, PAIR), BF16),
            pltpu.VMEM((BLOCKS, 128), F32),
            dma((DCHUNKS,)), dma((CHUNKS,)),
            dma((16,)), dma((16,)), dma((16,)), dma((16,)), dma((N_Z,)), dma((N_Z,)),
            dma((16,)), dma((16,)), dma((7,)), dma((7,)),
        ],
        compiler_params=pltpu.CompilerParams(collective_id=0, has_side_effects=True, vmem_limit_bytes=16000000),
        name="fused",
    )(*[pltpu.with_memory_space_constraint(a, pltpu.HBM) for a in operands])
    turned = pl.pallas_call(
        assemble,
        out_shape=jax.ShapeDtypeStruct((NSH, N_GZ * ROWSH * SHELL), F32),
        in_specs=[vmem],
        out_specs=vmem,
        scratch_shapes=[pltpu.VMEM((2, N_GZ * ROWSH * SHELL, 128), F32)],
        compiler_params=pltpu.CompilerParams(vmem_limit_bytes=16000000),
        name="assemble",
    )(got.reshape(2 * N_GZ * BLOCKS, 128))
    return turned.T


def solution(mesh):
    in_specs = (
        P(("gx", "gy", "gz"), None, None),
        P(("gx", "gy", "gz"), None),
        P(("gx", "gy", "gz"), None),
        P(("gx", "gy", "gz")),
        P("gy", None),
    )
    return jax.shard_map(shards, mesh=mesh, in_specs=in_specs, out_specs=P("gx", "gy"), check_vma=False)
```

```python
import jax
import jax.numpy as jnp
from jax import lax
from jax.experimental import pallas as pl
from jax.experimental.pallas import tpu as pltpu
from jax.sharding import PartitionSpec as P

SHELL = 16
PAIR = 256
TILES_DEV = 32
NSH = 192
N_GX = 8
N_Z = 8
N_GZ = 4
CAP = 8
ROWSH = 6
COLSH = 12
BLOCKS = ROWSH * COLSH
SLOTS = N_GX * CAP
CHUNKS = 2
DCHUNKS = 24
MESH = pl.DeviceIdType.MESH
F32 = jnp.float32
BF16 = jnp.bfloat16
I32 = jnp.int32


def order(rel):
    return max(0, min(2 * rel - 1, 2 * (N_GX - rel)))


def iota(shape, dim):
    return lax.broadcasted_iota(I32, shape, dim)


def fused(own_h, quart_h, sig_h, dens_hbm, eri_hbm, out_ref, own_s, quart_s, sig_s, isem, dens, eri, picked, vals, codes_out, held, ycode, zcode, mine, hots, half,
          dsem, esem, ysend, yrecv, ycsend, ycrecv, zcsend, zcrecv, rsend, rrecv, xsend, xrecv):
    gx, gy, gz = lax.axis_index("gx"), lax.axis_index("gy"), lax.axis_index("gz")
    z, core = gy // 2, lax.rem(gy, 2)

    def along_x(d, c):
        return {"gx": lax.rem(gx + N_GX - d, N_GX), "gy": z * 2 + c}

    def along_z(d):
        return {"gy": lax.rem(z + d + N_Z, N_Z) * 2 + core}

    def along_gz(d, c):
        return {"gy": z * 2 + c, "gz": lax.rem(gz + d + N_GZ, N_GZ)}

    mate = 1 - core
    step = 1 - 2 * core
    partner = {"gy": z * 2 + mate}
    ints = []
    for i, (src, dst) in enumerate(((own_h, own_s), (quart_h, quart_s), (sig_h, sig_s))):
        ints.append(pltpu.make_async_copy(src, dst, isem.at[i]))
        ints[-1].start()
    loads = []
    for c in range(DCHUNKS):
        loads.append(pltpu.make_async_copy(dens_hbm.at[:, :, pl.ds(c * 128, 128)], dens.at[pl.ds(c * COLSH, COLSH)], dsem.at[c]))
        loads[-1].start()
    per = TILES_DEV // CHUNKS
    copies = []
    for c in range(CHUNKS):
        part = pl.ds(c * per, per)
        copies.append(pltpu.make_async_copy(eri_hbm.at[part], eri.at[part], esem.at[c]))
        copies[-1].start()
    barrier = pltpu.get_barrier_semaphore()
    peers = [along_x(d, c) for d in range(1, N_GX) for c in range(2)] + [along_z(d) for d in range(1, N_Z)]
    peers += [along_gz(d, c) for d in (1, 2, 3) for c in range(2)] + [partner]
    for peer in peers[::-1]:
        pl.semaphore_signal(barrier, inc=1, device_id=peer, device_id_type=MESH)

    rows = TILES_DEV * SHELL
    lane = iota((1, 128), 1)
    tile = iota((1, rows), 1) >> 4
    codes = jnp.zeros((1, 128), I32)
    spread = jnp.zeros((1, rows), I32)
    counts = jnp.int32(0)
    places = []
    for c in ints:
        c.wait()
    for t in range(TILES_DEV):
        rel = (gx - own_s[0, t] + N_GX) & (N_GX - 1)
        row = jnp.maximum(0, jnp.minimum(2 * rel - 1, 2 * (N_GX - rel)))
        seen = (counts >> (row * 4)) & 15
        counts = counts + (jnp.int32(1) << (row * 4))
        slot = row * CAP + seen
        places.append(slot)
        codes = jnp.where(lane == row * 2 * CAP + core * CAP + seen, quart_s[0, t] * NSH + quart_s[1, t], codes)
        spread = jnp.where(tile == t, slot, spread)
    for i in range(N_GX):
        codes_out[i] = jnp.where((lane >> 4) == i, codes, 0)
    gather = (iota((128, rows), 0) == spread).astype(F32).astype(BF16)
    fold = ((iota((128, PAIR), 0) & 15) == (iota((128, PAIR), 1) & 15)).astype(F32).astype(BF16)
    for load in loads:
        load.wait()
    group = iota((SHELL, 128), 1) >> 4
    for t in range(TILES_DEV):
        shell = quart_s[3, t]
        block = dens[(shell >> 3) * COLSH + quart_s[2, t]].astype(F32)
        wanted = jnp.where(sig_s[0, t] != 0, shell & 7, -1)
        picked[t * SHELL:(t + 1) * SHELL, :] = jnp.where(group == wanted, block, 0.0)
    wide = jnp.dot(picked[...].astype(BF16), fold, preferred_element_type=F32)
    wide = jnp.where((iota((rows, PAIR), 0) & 15) == (iota((rows, PAIR), 1) >> 4), wide, 0.0).astype(BF16)
    flat = jnp.dot(gather, wide, preferred_element_type=F32)
    weights = flat[:SLOTS].astype(BF16)
    terms = jnp.zeros((SLOTS, PAIR), F32)
    slots = iota((SLOTS, PAIR), 0)
    group = 4
    for t in range(0, TILES_DEV, group):
        if t % per == 0:
            copies[t // per].wait()
        many = lax.dot_general(weights, eri[t:t + group].reshape(group * PAIR, PAIR), (((1,), (1,)), ((), ())), preferred_element_type=F32)
        for i in range(group):
            terms = jnp.where(slots == places[t + i], many[:, i * PAIR:(i + 1) * PAIR], terms)
    vals[0] = terms[:, :128]
    vals[1] = terms[:, 128:]
    held[0, pl.ds(pl.multiple_of(core * CAP, CAP), CAP), :] = jnp.where(core == 0, terms[:CAP, :128], terms[:CAP, 128:])

    pl.semaphore_wait(barrier, len(peers))

    def link(src, dst, s, r, peer):
        return pltpu.make_async_remote_copy(src_ref=src, dst_ref=dst, send_sem=s, recv_sem=r, device_id=peer, device_id_type=MESH)

    def send(src, dst, s, r, peer):
        copy = link(src, dst, s, r, peer)
        copy.start()
        started.append(copy)
        return copy

    started = []
    near = [1, 7, 2]
    far = [6, 3, 5, 4]

    def value_rows(r, c):
        return held.at[0, pl.ds(pl.multiple_of(r * 2 * CAP + c * CAP, CAP), CAP)]

    def give(r, c, peer):
        send(codes_out.at[r], ycode.at[r * 2 + core], ycsend.at[r * 2 + c], ycrecv.at[r * 2 + core], peer)
        send(vals.at[c, pl.ds(r * CAP, CAP)], value_rows(r, core), ysend.at[r * 2 + c], yrecv.at[r * 2 + core], peer)

    for d in far[::-1] + near[::-1]:
        for c in range(2):
            give(order(d), c, along_x(d, c))
    give(0, mate, partner)

    def value_in(r, c):
        link(vals.at[0, pl.ds(0, CAP)], value_rows(r, c), ysend.at[0], yrecv.at[r * 2 + c], partner).wait_recv()

    def code_in(r, c):
        link(codes_out.at[0], ycode.at[r * 2 + c], ycsend.at[0], ycrecv.at[r * 2 + c], partner).wait_recv()

    firsts, sizes = (0, 64), (64, 64)

    def hop(src, distance, dst, g):
        part = pl.ds(firsts[g], sizes[g])
        i = dst * 2 + g
        inward[dst, g] = send(held.at[src, part], held.at[dst, part], rsend.at[i], rrecv.at[i], along_z(distance))

    inward = {}
    rows = iota((2 * BLOCKS, 128), 0)
    other = (rows >= BLOCKS).astype(I32)
    inner = rows - other * BLOCKS
    bra = jnp.zeros_like(inner)
    for i in range(1, ROWSH):
        bra = bra + (inner >= i * COLSH).astype(I32)
    ket = inner - bra * COLSH
    column = jnp.where(other == 1, (z * 2 + 1 - core) * COLSH, gy * COLSH)
    wanted = bra * NSH + column + ket

    value_in(0, mate)
    for g, ds in enumerate(((1, 7, 2), (6, 3, 5, 4))):
        for d in ds:
            for c in range(2):
                value_in(order(d), c)
        hop(0, 2, 3, g)
        hop(0, -2, 4, g)
        hop(0, 1, 1, g)
        hop(0, -1, 2, g)
    code_in(0, mate)
    total = codes_out[0] + ycode[mate]
    for r in range(1, N_GX):
        for c in range(2):
            code_in(r, c)
            total = total + ycode[r * 2 + c]
    mine[...] = total
    zcode[0] = total
    zcode_in = []
    for d, slot in ((4, 7), (3, 5), (5, 6), (2, 3), (6, 4), (1, 1), (7, 2)):
        zcode_in.append(send(mine, zcode.at[slot], zcsend.at[slot], zcrecv.at[slot], along_z(d)))

    for g in range(2):
        inward[3, g].wait_recv()
        if g in (0,):
            hop(3, 2, 7, g)
        hop(3, 1, 5, g)
        inward[4, g].wait_recv()
        if g not in (0,):
            hop(4, -2, 7, g)
        hop(4, -1, 6, g)

    for c in zcode_in:
        c.wait_recv()
    early, late = (0, 3, 4, 1, 2), (5, 6, 7)
    for n, i in enumerate(early + late):
        hot = (wanted == zcode[i]).astype(F32).astype(BF16)
        hots[:, n * 256:n * 256 + 128] = hot
        hots[:, n * 256 + 128:n * 256 + 256] = hot

    def place(blocks, first):
        parts = []
        for i in blocks:
            top = held[i].astype(BF16)
            parts += [top, (held[i] - top.astype(F32)).astype(BF16)]
        return jnp.dot(hots[:, first * 256:(first + len(blocks)) * 256], jnp.concatenate(parts, axis=0), preferred_element_type=F32)

    for i in (1, 2):
        for g in range(2):
            inward[i, g].wait_recv()
    acc = place(early, 0)
    for i in late:
        for g in range(2):
            inward[i, g].wait_recv()
    acc = acc + place(late, len(early))
    half[...] = acc[BLOCKS:]
    out_ref[core, gz] = acc[:BLOCKS]

    home = out_ref.at[core, gz]

    def spread_out(i, src, peer):
        return send(src, home, xsend.at[i], xrecv.at[i], peer)

    last = [
        spread_out(6, half, partner),
        spread_out(4, home, along_gz(2, core)),
        spread_out(5, half, along_gz(2, mate)),
        spread_out(0, home, along_gz(step, core)),
        spread_out(1, half, along_gz(-step, mate)),
        spread_out(2, home, along_gz(-step, core)),
        spread_out(3, half, along_gz(step, mate)),
    ]
    for c in last:
        c.wait_recv()
    for c in started:
        c.wait_send()


def assemble(got_ref, out_ref, wide):
    group = iota((4 * ROWSH, 128), 1) >> 4
    pieces = [[got_ref[pl.ds(h * N_GZ * BLOCKS + k, 4 * ROWSH, stride=COLSH), :] for h in range(2)] for k in range(COLSH)]
    for a in range(SHELL):
        for j, ks in enumerate((range(8), range(8, COLSH))):
            line = jnp.zeros((4 * ROWSH, 128), F32)
            for k in ks:
                shift = ((k - a) % 8) * 16
                src = pieces[k][a // 8]
                moved = pltpu.roll(src, shift, 1) if shift else src
                line = jnp.where(group == k % 8, moved, line)
            wide[j, pl.ds(a, 4 * ROWSH, stride=SHELL), :] = line
    out_ref[:128, :] = wide[0].T
    out_ref[128:, :] = wide[1].T[:NSH - 128, :]


def shards(eri, owner, quartet, significance, density):
    hbm = pl.BlockSpec(memory_space=pltpu.HBM)
    vmem = pl.BlockSpec(memory_space=pltpu.VMEM)
    dma = pltpu.SemaphoreType.DMA
    operands = (owner.T, quartet.T, significance[None, :], density.reshape(COLSH, SHELL, density.shape[1]), eri)
    got = pl.pallas_call(
        fused,
        out_shape=jax.ShapeDtypeStruct((2, N_GZ, BLOCKS, 128), F32),
        in_specs=[hbm] * 5,
        out_specs=vmem,
        scratch_shapes=[
            pltpu.SMEM((1, TILES_DEV), I32),
            pltpu.SMEM((4, TILES_DEV), I32),
            pltpu.SMEM((1, TILES_DEV), I32),
            dma((3,)),
            pltpu.VMEM((DCHUNKS * COLSH, SHELL, 128), BF16),
            pltpu.VMEM(eri.shape, BF16),
            pltpu.VMEM((TILES_DEV * SHELL, 128), F32),
            pltpu.VMEM((2, SLOTS, 128), F32),
            pltpu.VMEM((N_GX, 1, 128), I32),
            pltpu.VMEM((N_Z, 2 * SLOTS, 128), F32),
            pltpu.VMEM((2 * N_GX, 1, 128), I32),
            pltpu.VMEM((N_Z, 1, 128), I32),
            pltpu.VMEM((1, 128), I32),
            pltpu.VMEM((2 * BLOCKS, N_Z * PAIR), BF16),
            pltpu.VMEM((BLOCKS, 128), F32),
            dma((DCHUNKS,)), dma((CHUNKS,)),
            dma((16,)), dma((16,)), dma((16,)), dma((16,)), dma((N_Z,)), dma((N_Z,)),
            dma((16,)), dma((16,)), dma((7,)), dma((7,)),
        ],
        compiler_params=pltpu.CompilerParams(collective_id=0, has_side_effects=True, vmem_limit_bytes=16000000),
        name="fused",
    )(*[pltpu.with_memory_space_constraint(a, pltpu.HBM) for a in operands])
    turned = pl.pallas_call(
        assemble,
        out_shape=jax.ShapeDtypeStruct((NSH, N_GZ * ROWSH * SHELL), F32),
        in_specs=[vmem],
        out_specs=vmem,
        scratch_shapes=[pltpu.VMEM((2, N_GZ * ROWSH * SHELL, 128), F32)],
        compiler_params=pltpu.CompilerParams(vmem_limit_bytes=16000000),
        name="assemble",
    )(got.reshape(2 * N_GZ * BLOCKS, 128))
    return turned.T


def solution(mesh):
    in_specs = (
        P(("gx", "gy", "gz"), None, None),
        P(("gx", "gy", "gz"), None),
        P(("gx", "gy", "gz"), None),
        P(("gx", "gy", "gz")),
        P("gy", None),
    )
    return jax.shard_map(shards, mesh=mesh, in_specs=in_specs, out_specs=P("gx", "gy"), check_vma=False)
```

```python
import jax
import jax.numpy as jnp
from jax import lax
from jax.experimental import pallas as pl
from jax.experimental.pallas import tpu as pltpu
from jax.sharding import PartitionSpec as P

SHELL = 16
PAIR = 256
TILES_DEV = 32
NSH = 192
N_GX = 8
N_Z = 8
N_GZ = 4
CAP = 8
ROWSH = 6
COLSH = 12
BLOCKS = ROWSH * COLSH
SLOTS = N_GX * CAP
CHUNKS = 2
DCHUNKS = 24
MESH = pl.DeviceIdType.MESH
F32 = jnp.float32
BF16 = jnp.bfloat16
I32 = jnp.int32


def order(rel):
    return max(0, min(2 * rel - 1, 2 * (N_GX - rel)))


def iota(shape, dim):
    return lax.broadcasted_iota(I32, shape, dim)


def fused(own_h, quart_h, sig_h, dens_hbm, eri_hbm, out_ref, own_s, quart_s, sig_s, isem, dens, eri, picked, vals, codes_out, held, ycode, zcode, mine, hots, half,
          dsem, esem, ysend, yrecv, ycsend, ycrecv, zcsend, zcrecv, rsend, rrecv, xsend, xrecv):
    gx, gy, gz = lax.axis_index("gx"), lax.axis_index("gy"), lax.axis_index("gz")
    z, core = gy // 2, lax.rem(gy, 2)

    def along_x(d, c):
        return {"gx": lax.rem(gx + N_GX - d, N_GX), "gy": z * 2 + c}

    def along_z(d):
        return {"gy": lax.rem(z + d + N_Z, N_Z) * 2 + core}

    def along_gz(d, c):
        return {"gy": z * 2 + c, "gz": lax.rem(gz + d + N_GZ, N_GZ)}

    mate = 1 - core
    step = 1 - 2 * core
    partner = {"gy": z * 2 + mate}
    ints = []
    for i, (src, dst) in enumerate(((own_h, own_s), (quart_h, quart_s), (sig_h, sig_s))):
        ints.append(pltpu.make_async_copy(src, dst, isem.at[i]))
        ints[-1].start()
    loads = []
    for c in range(DCHUNKS):
        loads.append(pltpu.make_async_copy(dens_hbm.at[:, :, pl.ds(c * 128, 128)], dens.at[pl.ds(c * COLSH, COLSH)], dsem.at[c]))
        loads[-1].start()
    per = TILES_DEV // CHUNKS
    copies = []
    for c in range(CHUNKS):
        part = pl.ds(c * per, per)
        copies.append(pltpu.make_async_copy(eri_hbm.at[part], eri.at[part], esem.at[c]))
        copies[-1].start()
    barrier = pltpu.get_barrier_semaphore()
    peers = [along_x(d, c) for d in range(1, N_GX) for c in range(2)] + [along_z(d) for d in range(1, N_Z)]
    peers += [along_gz(d, c) for d in (1, 2, 3) for c in range(2)] + [partner]
    for peer in peers[::-1]:
        pl.semaphore_signal(barrier, inc=1, device_id=peer, device_id_type=MESH)

    rows = TILES_DEV * SHELL
    lane = iota((1, 128), 1)
    tile = iota((1, rows), 1) >> 4
    codes = jnp.zeros((1, 128), I32)
    spread = jnp.zeros((1, rows), I32)
    counts = jnp.int32(0)
    places = []
    for c in ints:
        c.wait()
    for t in range(TILES_DEV):
        rel = (gx - own_s[0, t] + N_GX) & (N_GX - 1)
        row = jnp.maximum(0, jnp.minimum(2 * rel - 1, 2 * (N_GX - rel)))
        seen = (counts >> (row * 4)) & 15
        counts = counts + (jnp.int32(1) << (row * 4))
        slot = row * CAP + seen
        places.append(slot)
        codes = jnp.where(lane == row * 2 * CAP + core * CAP + seen, quart_s[0, t] * NSH + quart_s[1, t], codes)
        spread = jnp.where(tile == t, slot, spread)
    for i in range(N_GX):
        codes_out[i] = jnp.where((lane >> 4) == i, codes, 0)
    gather = (iota((128, rows), 0) == spread).astype(F32).astype(BF16)
    fold = ((iota((128, PAIR), 0) & 15) == (iota((128, PAIR), 1) & 15)).astype(F32).astype(BF16)
    for load in loads:
        load.wait()
    group = iota((SHELL, 128), 1) >> 4
    for t in range(TILES_DEV):
        shell = quart_s[3, t]
        block = dens[(shell >> 3) * COLSH + quart_s[2, t]].astype(F32)
        wanted = jnp.where(sig_s[0, t] != 0, shell & 7, -1)
        picked[t * SHELL:(t + 1) * SHELL, :] = jnp.where(group == wanted, block, 0.0)
    wide = jnp.dot(picked[...].astype(BF16), fold, preferred_element_type=F32)
    wide = jnp.where((iota((rows, PAIR), 0) & 15) == (iota((rows, PAIR), 1) >> 4), wide, 0.0).astype(BF16)
    flat = jnp.dot(gather, wide, preferred_element_type=F32)
    weights = flat[:SLOTS].astype(BF16)
    terms = jnp.zeros((SLOTS, PAIR), F32)
    slots = iota((SLOTS, PAIR), 0)
    group = 4
    for t in range(0, TILES_DEV, group):
        if t % per == 0:
            copies[t // per].wait()
        many = lax.dot_general(weights, eri[t:t + group].reshape(group * PAIR, PAIR), (((1,), (1,)), ((), ())), preferred_element_type=F32)
        for i in range(group):
            terms = jnp.where(slots == places[t + i], many[:, i * PAIR:(i + 1) * PAIR], terms)
    vals[0] = terms[:, :128]
    vals[1] = terms[:, 128:]
    held[0, pl.ds(pl.multiple_of(core * CAP, CAP), CAP), :] = jnp.where(core == 0, terms[:CAP, :128], terms[:CAP, 128:])

    pl.semaphore_wait(barrier, len(peers))

    def link(src, dst, s, r, peer):
        return pltpu.make_async_remote_copy(src_ref=src, dst_ref=dst, send_sem=s, recv_sem=r, device_id=peer, device_id_type=MESH)

    def send(src, dst, s, r, peer):
        copy = link(src, dst, s, r, peer)
        copy.start()
        started.append(copy)
        return copy

    started = []
    near = [1, 7, 2]
    far = [6, 3, 5, 4]

    def value_rows(r, c):
        return held.at[0, pl.ds(pl.multiple_of(r * 2 * CAP + c * CAP, CAP), CAP)]

    def give(r, c, peer):
        send(codes_out.at[r], ycode.at[r * 2 + core], ycsend.at[r * 2 + c], ycrecv.at[r * 2 + core], peer)
        send(vals.at[c, pl.ds(r * CAP, CAP)], value_rows(r, core), ysend.at[r * 2 + c], yrecv.at[r * 2 + core], peer)

    for d in far[::-1] + near[::-1]:
        for c in range(2):
            give(order(d), c, along_x(d, c))
    give(0, mate, partner)

    def value_in(r, c):
        link(vals.at[0, pl.ds(0, CAP)], value_rows(r, c), ysend.at[0], yrecv.at[r * 2 + c], partner).wait_recv()

    def code_in(r, c):
        link(codes_out.at[0], ycode.at[r * 2 + c], ycsend.at[0], ycrecv.at[r * 2 + c], partner).wait_recv()

    firsts, sizes = (0, 64), (64, 64)

    def hop(src, distance, dst, g):
        part = pl.ds(firsts[g], sizes[g])
        i = dst * 2 + g
        inward[dst, g] = send(held.at[src, part], held.at[dst, part], rsend.at[i], rrecv.at[i], along_z(distance))

    inward = {}
    rows = iota((2 * BLOCKS, 128), 0)
    other = (rows >= BLOCKS).astype(I32)
    inner = rows - other * BLOCKS
    bra = jnp.zeros_like(inner)
    for i in range(1, ROWSH):
        bra = bra + (inner >= i * COLSH).astype(I32)
    ket = inner - bra * COLSH
    column = jnp.where(other == 1, (z * 2 + 1 - core) * COLSH, gy * COLSH)
    wanted = bra * NSH + column + ket

    value_in(0, mate)
    for g, ds in enumerate(((1, 7, 2), (6, 3, 5, 4))):
        for d in ds:
            for c in range(2):
                value_in(order(d), c)
        hop(0, 2, 3, g)
        hop(0, -2, 4, g)
        hop(0, 1, 1, g)
        hop(0, -1, 2, g)
    code_in(0, mate)
    total = codes_out[0] + ycode[mate]
    for r in range(1, N_GX):
        for c in range(2):
            code_in(r, c)
            total = total + ycode[r * 2 + c]
    mine[...] = total
    zcode[0] = total
    zcode_in = []
    for d, slot in ((4, 7), (3, 5), (5, 6), (2, 3), (6, 4), (1, 1), (7, 2)):
        zcode_in.append(send(mine, zcode.at[slot], zcsend.at[slot], zcrecv.at[slot], along_z(d)))

    for g in range(2):
        inward[3, g].wait_recv()
        if g in (0,):
            hop(3, 2, 7, g)
        hop(3, 1, 5, g)
        inward[4, g].wait_recv()
        if g not in (0,):
            hop(4, -2, 7, g)
        hop(4, -1, 6, g)

    for c in zcode_in:
        c.wait_recv()
    early, late = (0, 3, 4, 1, 2), (5, 6, 7)
    for n, i in enumerate(early + late):
        hot = (wanted == zcode[i]).astype(F32).astype(BF16)
        hots[:, n * 256:n * 256 + 128] = hot
        hots[:, n * 256 + 128:n * 256 + 256] = hot

    def place(blocks, first):
        parts = []
        for i in blocks:
            top = held[i].astype(BF16)
            parts += [top, (held[i] - top.astype(F32)).astype(BF16)]
        return jnp.dot(hots[:, first * 256:(first + len(blocks)) * 256], jnp.concatenate(parts, axis=0), preferred_element_type=F32)

    for i in (1, 2):
        for g in range(2):
            inward[i, g].wait_recv()
    acc = place(early, 0)
    for n, blocks in ((5, (5, 6)), (7, (7,))):
        for i in blocks:
            for g in range(2):
                inward[i, g].wait_recv()
        acc = acc + place(blocks, n)
    half[...] = acc[BLOCKS:]
    home = out_ref.at[core, gz]

    def spread_out(i, src, peer):
        return send(src, home, xsend.at[i], xrecv.at[i], peer)

    last = [
        spread_out(5, half, along_gz(2, mate)),
        spread_out(6, half, partner),
        spread_out(1, half, along_gz(-step, mate)),
        spread_out(3, half, along_gz(step, mate)),
    ]
    out_ref[core, gz] = acc[:BLOCKS]
    last += [
        spread_out(4, home, along_gz(2, core)),
        spread_out(0, home, along_gz(step, core)),
        spread_out(2, home, along_gz(-step, core)),
    ]
    for c in last:
        c.wait_recv()
    for c in started:
        c.wait_send()


def assemble(got_ref, out_ref, wide):
    group = iota((4 * ROWSH, 128), 1) >> 4
    pieces = [[got_ref[pl.ds(h * N_GZ * BLOCKS + k, 4 * ROWSH, stride=COLSH), :] for h in range(2)] for k in range(COLSH)]
    for a in range(SHELL):
        for j, ks in enumerate((range(8), range(8, COLSH))):
            line = jnp.zeros((4 * ROWSH, 128), F32)
            for k in ks:
                shift = ((k - a) % 8) * 16
                src = pieces[k][a // 8]
                moved = pltpu.roll(src, shift, 1) if shift else src
                line = jnp.where(group == k % 8, moved, line)
            wide[j, pl.ds(a, 4 * ROWSH, stride=SHELL), :] = line
    out_ref[:128, :] = wide[0].T
    out_ref[128:, :] = wide[1].T[:NSH - 128, :]


def shards(eri, owner, quartet, significance, density):
    hbm = pl.BlockSpec(memory_space=pltpu.HBM)
    vmem = pl.BlockSpec(memory_space=pltpu.VMEM)
    dma = pltpu.SemaphoreType.DMA
    operands = (owner.T, quartet.T, significance[None, :], density.reshape(COLSH, SHELL, density.shape[1]), eri)
    got = pl.pallas_call(
        fused,
        out_shape=jax.ShapeDtypeStruct((2, N_GZ, BLOCKS, 128), F32),
        in_specs=[hbm] * 5,
        out_specs=vmem,
        scratch_shapes=[
            pltpu.SMEM((1, TILES_DEV), I32),
            pltpu.SMEM((4, TILES_DEV), I32),
            pltpu.SMEM((1, TILES_DEV), I32),
            dma((3,)),
            pltpu.VMEM((DCHUNKS * COLSH, SHELL, 128), BF16),
            pltpu.VMEM(eri.shape, BF16),
            pltpu.VMEM((TILES_DEV * SHELL, 128), F32),
            pltpu.VMEM((2, SLOTS, 128), F32),
            pltpu.VMEM((N_GX, 1, 128), I32),
            pltpu.VMEM((N_Z, 2 * SLOTS, 128), F32),
            pltpu.VMEM((2 * N_GX, 1, 128), I32),
            pltpu.VMEM((N_Z, 1, 128), I32),
            pltpu.VMEM((1, 128), I32),
            pltpu.VMEM((2 * BLOCKS, N_Z * PAIR), BF16),
            pltpu.VMEM((BLOCKS, 128), F32),
            dma((DCHUNKS,)), dma((CHUNKS,)),
            dma((16,)), dma((16,)), dma((16,)), dma((16,)), dma((N_Z,)), dma((N_Z,)),
            dma((16,)), dma((16,)), dma((7,)), dma((7,)),
        ],
        compiler_params=pltpu.CompilerParams(collective_id=0, has_side_effects=True, vmem_limit_bytes=16000000),
        name="fused",
    )(*[pltpu.with_memory_space_constraint(a, pltpu.HBM) for a in operands])
    turned = pl.pallas_call(
        assemble,
        out_shape=jax.ShapeDtypeStruct((NSH, N_GZ * ROWSH * SHELL), F32),
        in_specs=[vmem],
        out_specs=vmem,
        scratch_shapes=[pltpu.VMEM((2, N_GZ * ROWSH * SHELL, 128), F32)],
        compiler_params=pltpu.CompilerParams(vmem_limit_bytes=16000000),
        name="assemble",
    )(got.reshape(2 * N_GZ * BLOCKS, 128))
    return turned.T


def solution(mesh):
    in_specs = (
        P(("gx", "gy", "gz"), None, None),
        P(("gx", "gy", "gz"), None),
        P(("gx", "gy", "gz"), None),
        P(("gx", "gy", "gz")),
        P("gy", None),
    )
    return jax.shard_map(shards, mesh=mesh, in_specs=in_specs, out_specs=P("gx", "gy"), check_vma=False)
```
